32 devices in a mesh: dp: 8 (over z, y), mp: 4 (over x, core).
Axes of the slice: x: 2, y: 2, z: 4, core: 2. Of those that a mesh axis runs over, the one named last changes fastest.
Arguments:
- features: bfloat16 [3, 512, 16384], P(None, 'mp', 'dp'), may hold values from -6 to 6
- weights: bfloat16 [11, 512, 512], P(None, 'mp'), may hold values from -0.25 to 0.25
- sample_owner: int32 [3, 16384, 1], P(None, 'dp'), may hold values from 0 to 7; in each aligned block of 2048 rows (0 to 2047, 2048 to 4095, ..., all dimensions but the last counted through in order) at most 512 rows name the same one
- sample_row: int32 [3, 16384], P(None, 'dp'), may hold values from 0 to 2047
- edge_src: int32 [8, 16384], P(None, 'dp'), may hold values from 0 to 2047
- edge_dst: int32 [8, 16384], P(None, 'dp'), may hold values from 0 to 127
- edge_count: int32 [8, 8], P(None, 'dp'), may hold values from 128 to 2048
Outputs:
- updated: bfloat16 [3, 512, 1024], P(None, 'mp', 'dp')
The draws below stay inside these ranges and needn't reach their ends.
Inputs may be any that keep to these rules, and one draw needn't show every extreme that they name: `sample_owner`: among the 2048 entries of one node type in one block no owner appears more than 512 times; some owner appears exactly 512 times in some blocks.
All inputs are finite; a program needn't handle non-finite values.
Results may differ from the reference program's by a relative error of at most 0.0064.
Values may be sent and summed in bfloat16 or wider, within the bound.
A program may use at most 64 MiB of HBM per device.

```python
import math
import jax
import jax.numpy as jnp
import numpy as np
from jax import lax

D = 512
RELS = 8
TYPES = 3
MATS = 11
ROWS_DEV = 2048
SAMP = 2048
SEEDS = 128
EDGES = 2048
CAP = 512
TABLE_ROWS = 16384
SAMPLES = 16384
EDGES_ALL = 16384
N_DP = 8


def plant(values, stream_key, smallest, high):
    extent = values.shape
    spot = [jax.random.randint(jax.random.fold_in(stream_key, axis), (), 0, extent[axis]) for axis in range(len(extent))]
    values = values.at[tuple(spot)].set(smallest)
    longest = extent.index(max(extent))
    spot[longest] = (spot[longest] + 1) % extent[longest]
    return values.at[tuple(spot)].set(high)


def level_of(rng, shape, cuts, low, largest):
    loudness = 1.0
    for position, shards_of in cuts:
        draws = jax.random.uniform(jax.random.fold_in(jax.random.fold_in(rng, 6), position), (shards_of,), jnp.float32, low / len(cuts), largest / len(cuts))
        loudness = loudness * jnp.repeat(jnp.exp(draws), shape[position] // shards_of).reshape((-1,) + (1,) * (len(shape) - 1 - position))
    return loudness


def assign_block(own_key, own, number, rows, count, top, limit, lean):
    sequence = jax.random.permutation(own_key, count)
    heavy_load, common = portions_of(count, rows * top, limit, lean, True), portions_of(count, rows * top, limit, lean, False)
    places = jnp.arange(count)

    def named(tallies, rotation):
        used = int((tallies > 0).sum())
        fixed = max(1, used // 4)
        passed = fixed + (places - fixed + rotation * (used - fixed)) % max(1, count - fixed)
        return jnp.zeros((count,), jnp.int32).at[sequence[jnp.where(places < fixed, places, passed)]].set(jnp.asarray(tallies, jnp.int32))

    tallies = jnp.where(number % 4 == 0, named(heavy_load, number // 4), named(common, number - number // 4 - 1))
    mixed = jax.random.permutation(jax.random.fold_in(own, 3), count)
    source_of, sink = mixed[0:count // 2 * 2:2], mixed[1:count // 2 * 2:2]
    margin = jnp.minimum(tallies[source_of] - 1, limit - tallies[sink]) // 2
    margin = jnp.where((source_of == sequence[0]) | (sink == sequence[0]) | (tallies[sink] == 0), 0, jnp.maximum(margin, 0))
    passed = jax.random.randint(jax.random.fold_in(own, 4), (count // 2,), 0, 1 << 20) % (margin + 1)
    tallies = tallies.at[source_of].add(-passed).at[sink].add(passed)
    labels = jnp.searchsorted(jnp.cumsum(tallies), jnp.arange(rows * top), side="right").astype(jnp.int32)
    listing = labels.reshape(top, rows).T
    listing = listing[jax.random.permutation(jax.random.fold_in(own, 1), rows)]
    rotation = jax.random.randint(jax.random.fold_in(own, 2), (rows, 1), 0, top)
    return jnp.take_along_axis(listing, (jnp.arange(top)[None, :] + rotation) % top, axis=1)


def portions_of(count, total, limit, skew, full):
    loads = [(1 << 20) // math.isqrt(standing ** skew) + 1 for standing in range(1, count + 1)]
    largest = limit if full else min(limit, max(-(-total // count), total * loads[0] // sum(loads)))
    least = 1 if total - largest >= count - 1 else 0
    given, rest = [largest] + [least] * (count - 1), total - largest - least * (count - 1)
    while rest > 0:
        free = [i for i in range(1, count) if given[i] < largest] or [i for i in range(1, count) if given[i] < limit]
        whole, left = sum([loads[i] for i in free]), rest
        for i in free:
            more = min(limit - given[i], max(1, left * loads[i] // whole), rest)
            given[i] = given[i] + more
            rest = rest - more
    return np.array(given)


def normal_values(key, dims, width, most, split=(), kind=jnp.bfloat16):
    drawn = jax.random.normal(key, dims, jnp.float32) * width
    if len(split) > 0:
        drawn = level_of(key, dims, split, -0.22, 0.18) * drawn
    return jnp.clip(drawn, min=-most, max=most).astype(kind)


def setup_inputs(seed: int = 0) -> dict:
    arg_keys = jax.random.split(jax.random.key(seed), 8)
    features = normal_values(arg_keys[0], (TYPES, D, TABLE_ROWS), 1.0, 6.0, ((1, 4), (2, 8)))
    weights = normal_values(arg_keys[1], (MATS, D, D), D ** -0.5, 0.25, ((1, 4),))
    sample_owner_keys = jax.random.split(jax.random.fold_in(arg_keys[2], 1), TYPES * SAMPLES // SAMP)
    sample_owner_turns = jax.random.permutation(jax.random.fold_in(arg_keys[2], 3), TYPES * SAMPLES // SAMP)
    sample_owner = jax.vmap(lambda own, number: assign_block(jax.random.fold_in(arg_keys[2], 2), own, number, SAMP, N_DP, 1, CAP, 2))(sample_owner_keys, sample_owner_turns).reshape((TYPES, SAMPLES, 1))
    sample_row = plant(jax.random.randint(arg_keys[3], (TYPES, SAMPLES), 0, ROWS_DEV), jax.random.fold_in(arg_keys[3], 1), 0, ROWS_DEV - 1).astype(jnp.int32)
    edge_src = plant(jax.random.randint(arg_keys[4], (RELS, EDGES_ALL), 0, SAMP), jax.random.fold_in(arg_keys[4], 1), 0, SAMP - 1).astype(jnp.int32)
    edge_dst = plant(jax.random.randint(arg_keys[5], (RELS, EDGES_ALL), 0, SEEDS), jax.random.fold_in(arg_keys[5], 1), 0, SEEDS - 1).astype(jnp.int32)
    edge_count = plant(jax.random.randint(arg_keys[6], (RELS, N_DP), EDGES // 16, EDGES + 1), jax.random.fold_in(arg_keys[6], 1), EDGES // 16, EDGES).astype(jnp.int32)
    return {"features": features, "weights": weights, "sample_owner": sample_owner, "sample_row": sample_row, "edge_src": edge_src, "edge_dst": edge_dst, "edge_count": edge_count}


RELATION_SOURCE = (0, 1, 0, 1, 2, 0, 2, 1)
RELATION_TARGET = (1, 0, 0, 2, 1, 2, 0, 1)


def reference(features, weights, sample_owner, sample_row, edge_src, edge_dst, edge_count):
    row_index = (sample_owner[:, :, 0] * ROWS_DEV + sample_row).astype(jnp.int32)
    block_index = row_index.reshape(TYPES, N_DP, SAMP).transpose(1, 0, 2)
    block_src = edge_src.reshape(RELS, N_DP, EDGES).transpose(1, 0, 2)
    block_dst = edge_dst.reshape(RELS, N_DP, EDGES).transpose(1, 0, 2)
    block_count = edge_count.transpose(1, 0)

    def one_block(inputs):
        index_here, src_here, dst_here, count_here = inputs
        fetched = [jnp.take(features[node_kind], index_here[node_kind], axis=1).T for node_kind in range(TYPES)]
        typed = [jnp.dot(fetched[node_kind][:SEEDS], weights[RELS + node_kind], preferred_element_type=jnp.float32) for node_kind in range(TYPES)]
        slot_ids = jnp.arange(EDGES, dtype=jnp.int32)
        for relation in range(RELS):
            live_edge = (slot_ids < count_here[relation]).astype(jnp.float32)
            sources = jnp.take(fetched[RELATION_SOURCE[relation]], src_here[relation], axis=0).astype(jnp.float32)
            summed = jax.ops.segment_sum(sources * live_edge[:, None], dst_here[relation], num_segments=SEEDS)
            degree = jax.ops.segment_sum(live_edge, dst_here[relation], num_segments=SEEDS)
            message = (summed / jnp.maximum(degree, 1.0)[:, None]).astype(jnp.bfloat16)
            target = RELATION_TARGET[relation]
            typed[target] = typed[target] + jnp.dot(message, weights[relation], preferred_element_type=jnp.float32)
        return jnp.stack([jax.nn.relu(value).astype(jnp.bfloat16) for value in typed])

    result = lax.map(one_block, (block_index, block_src, block_dst, block_count))
    return result.transpose(1, 3, 0, 2).reshape(TYPES, result.shape[3], N_DP * SEEDS)
```

```python
import functools

import jax
import jax.numpy as jnp
from jax import lax
from jax.experimental import pallas as pl
from jax.experimental.pallas import tpu as pltpu
from jax.sharding import PartitionSpec as P

SEEDS = 128
RELATION_SOURCE = (0, 1, 0, 1, 2, 0, 2, 1)
MATRIX_TARGET = (1, 0, 0, 2, 1, 2, 0, 1, 0, 1, 2)
RELS = len(RELATION_SOURCE)
KINDS = 3
MATS = RELS + KINDS
SLOTS = tuple(
    tuple([r for r in range(RELS) if RELATION_SOURCE[r] == k] + [RELS + k]) for k in range(KINDS)
)
ORDER = tuple(m for group in SLOTS for m in group)
STARTS = tuple(sum(len(group) for group in SLOTS[:k]) for k in range(KINDS))
HALVES = 2
STEP = 256
MESH = pl.DeviceIdType.MESH
NT = (((1,), (1,)), ((), ()))
TN = (((0,), (0,)), ((), ()))


def log2(n):
    return n.bit_length() - 1


def kernel(groups, shares, features, weights, owner, row, src, dst, count, out,
           iota, tab, req_send, req_recv, pos, edges, send, recv, adj, deg, part,
           part_send, part_recv, typed, typed_send, typed_recv,
           req_ss, req_rs, idx_ss, idx_rs, row_ss, row_rs, part_ss, part_rs, typed_ss, typed_rs):
    kinds, feat, rows = features.shape
    sampled = owner.shape[1]
    edge_total = src.shape[1]
    cap = req_send.shape[2]
    low = tab.shape[2]
    high = rows // low
    s_high = sampled // low
    side = groups // HALVES
    g = lax.axis_index("dp")
    m = lax.axis_index("mp")
    half = g // side
    q = lax.rem(g, side)
    f32, bf16, i32 = jnp.float32, jnp.bfloat16, jnp.int32

    def one_hot(index, size):
        n = index.shape[1]
        pieces = []
        for base in range(0, size, STEP):
            span = min(STEP, size - base)
            local = index - base
            local = jnp.where((local >= 0) & (local < span), local, -1).astype(f32).astype(bf16)
            hit = iota[:span, :n] == local
            pieces.append(jnp.where(hit, jnp.ones((), bf16), jnp.zeros((), bf16)))
        return pieces[0] if len(pieces) == 1 else jnp.concatenate(pieces, axis=0)

    barrier = pltpu.get_barrier_semaphore()
    for d in range(1, groups):
        pl.semaphore_signal(barrier, inc=1, device_id={"dp": lax.rem(g + d, groups)}, device_id_type=MESH)
    for d in range(1, shares):
        pl.semaphore_signal(barrier, inc=1, device_id={"mp": lax.rem(m + d, shares)}, device_id_type=MESH)

    iota[...] = lax.broadcasted_iota(i32, iota.shape, 0).astype(f32).astype(bf16)
    tri = (lax.broadcasted_iota(i32, (STEP, STEP), 0) <= lax.broadcasted_iota(i32, (STEP, STEP), 1))
    tri = jnp.where(tri, 1.0, 0.0).astype(bf16)
    for k in range(kinds):
        owners = owner[k:k + 1, :]
        hot = jnp.where(lax.broadcasted_iota(i32, (groups, sampled), 0) == owners, 1.0, 0.0)
        carry = jnp.zeros((groups, 1), f32)
        ranks = []
        for base in range(0, sampled, STEP):
            piece = hot[:, base:base + STEP]
            upto = jnp.dot(piece.astype(bf16), tri, preferred_element_type=f32) + carry
            ranks.append(jnp.sum((upto - 1.0) * piece, axis=0, keepdims=True))
            carry = carry + jnp.sum(piece, axis=1, keepdims=True)
        rank = jnp.concatenate(ranks, axis=1).astype(i32)
        pos[half, k:k + 1, :] = owners * cap + rank
        wanted = row[k:k + 1, :]
        coarse = hot * (wanted >> 8).astype(f32)
        fine = hot * (wanted & 255).astype(f32)
        pair = jnp.concatenate([coarse, fine], axis=0).astype(bf16)
        listed = lax.dot_general(pair, one_hot(rank, cap), NT, preferred_element_type=f32)
        listed = (listed[:groups] * 256.0 + listed[groups:]).astype(i32)
        for o in range(groups):
            req_send[o, k:k + 1, :] = listed[o:o + 1]
    slots = lax.broadcasted_iota(i32, (RELS, edge_total), 1)
    edges[half] = jnp.where(slots < count[...], dst[...] * sampled + src[...], -1)

    pl.semaphore_wait(barrier, groups - 1 + shares - 1)
    asks = []
    for d in range(1, groups):
        to = lax.rem(g + d, groups)
        copy = pltpu.make_async_remote_copy(
            req_send.at[to], req_recv.at[g], req_ss.at[d], req_rs.at[d],
            device_id={"dp": to}, device_id_type=MESH)
        copy.start()
        asks.append(copy)
    hints = []
    for i in range(1, HALVES):
        to = lax.rem(half + i, HALVES) * side + q
        for n, ref in enumerate((pos, edges)):
            copy = pltpu.make_async_remote_copy(
                ref.at[half], ref.at[half], idx_ss.at[i, n], idx_rs.at[i, n],
                device_id={"dp": to}, device_id_type=MESH)
            copy.start()
            hints.append(copy)

    for k in range(kinds):
        for h in range(high):
            tab[k, h * feat:(h + 1) * feat, :] = features[k, :, h * low:(h + 1) * low]

    def build(i, lo_r, hi_r):
        block = lax.rem(half + i, HALVES)

        def one(r, _):
            packed = edges[block, pl.ds(r, 1), :]
            live = packed >= 0
            source = packed & (sampled - 1)
            left = one_hot(jnp.where(live, source & (low - 1), -1), low)
            column = (source >> log2(low)) * SEEDS + (packed >> log2(sampled))
            right = one_hot(jnp.where(live, column, -1), s_high * SEEDS)
            counts = lax.dot_general(left, right, NT, preferred_element_type=f32)
            adj[i, r] = counts.astype(bf16)
            total = jnp.sum(counts, axis=0, keepdims=True)
            seen = total[:, :SEEDS]
            for h in range(1, s_high):
                seen = seen + total[:, h * SEEDS:(h + 1) * SEEDS]
            deg[i, r] = jnp.broadcast_to(jnp.maximum(seen, 1.0), (8, SEEDS))
            return 0

        lax.fori_loop(lo_r, hi_r, one, 0)

    build(0, 0, 2)
    req_recv[g] = req_send[g]
    for copy in asks:
        copy.wait()

    def pick(k, block):
        wanted = req_recv[block, k:k + 1, :]
        found = jnp.dot(tab[k], one_hot(wanted & (low - 1), low), preferred_element_type=f32)
        bank = wanted >> log2(low)
        chosen = jnp.zeros((feat, cap), f32)
        for h in range(high):
            chosen = jnp.where(bank == h, found[h * feat:(h + 1) * feat], chosen)
        return chosen.astype(bf16)

    def row_copy(k, d, j):
        return pltpu.make_async_remote_copy(
            send.at[k, d, j], recv.at[k, j, q], row_ss.at[k, d, j], row_rs.at[k, d, j],
            device_id={"dp": half * side + lax.rem(q + d, side)}, device_id_type=MESH)

    for k in range(kinds):
        def serve(n, _, k=k):
            d, j = 1 + n // HALVES, lax.rem(n, HALVES)
            send[k, d, j] = pick(k, j * side + lax.rem(q + d, side))
            row_copy(k, d, j).start()
            return 0

        lax.fori_loop(0, (side - 1) * HALVES, serve, 0)
    for k in range(kinds):
        def keep(j, _, k=k):
            recv[k, j, q] = pick(k, j * side + q)
            return 0

        lax.fori_loop(0, HALVES, keep, 0)

    build(0, 2, RELS)
    for copy in hints:
        copy.wait()
    for i in range(1, HALVES):
        build(i, 0, RELS)

    replies = []
    for k in range(kinds):
        start, size = STARTS[k], len(SLOTS[k])

        def landed(n, _, k=k):
            row_copy(k, 1 + n // HALVES, lax.rem(n, HALVES)).wait()
            return 0

        lax.fori_loop(0, (side - 1) * HALVES, landed, 0)
        for i in reversed(range(HALVES)):
            block = lax.rem(half + i, HALVES)
            sums = [jnp.zeros((feat, SEEDS), f32) for _ in SLOTS[k][:-1]]
            stack = recv[k, block].reshape(side * feat, cap)
            for h in range(s_high):
                where = pos[block, k:k + 1, h * low:(h + 1) * low]
                found = jnp.dot(stack, one_hot(where & (cap - 1), cap), preferred_element_type=f32)
                holder = (where >> log2(cap)) - half * side
                chosen = jnp.zeros((feat, low), f32)
                for o in range(side):
                    chosen = jnp.where(holder == o, found[o * feat:(o + 1) * feat], chosen)
                chosen = chosen.astype(bf16)
                if h == 0:
                    own = chosen[:, :SEEDS].astype(f32)
                for n, r in enumerate(SLOTS[k][:-1]):
                    sums[n] = sums[n] + jnp.dot(
                        chosen, adj[i, r, :, h * SEEDS:(h + 1) * SEEDS], preferred_element_type=f32)
            values = [value / deg[i, r][:1] for value, r in zip(sums, SLOTS[k][:-1])] + [own]
            for n, value in enumerate(values):
                if i == 0:
                    part[start + n] = value
                else:
                    part_send[i, start + n] = value.astype(bf16)
            if i > 0:
                copy = pltpu.make_async_remote_copy(
                    part_send.at[i, pl.ds(start, size)], part_recv.at[i, pl.ds(start, size)],
                    part_ss.at[i, k], part_rs.at[i, k],
                    device_id={"dp": block * side + q}, device_id_type=MESH)
                copy.start()
                replies.append(copy)
    for copy in replies:
        copy.wait()

    sums = [jnp.zeros((SEEDS, weights.shape[2]), f32) for _ in range(kinds)]
    for n, matrix in enumerate(ORDER):
        message = part[n]
        for i in range(1, HALVES):
            message = message + part_recv[i, n].astype(f32)
        target = MATRIX_TARGET[matrix]
        sums[target] = sums[target] + lax.dot_general(
            message.astype(bf16), weights[matrix], TN, preferred_element_type=f32)
    width = typed.shape[3]
    for t in range(kinds):
        for p in range(shares):
            piece = sums[t][:, p * width:(p + 1) * width]
            typed[p, t] = piece
            typed_send[p, t] = piece.astype(bf16)
    last = []
    for d in range(1, shares):
        to = lax.rem(m + d, shares)
        copy = pltpu.make_async_remote_copy(
            typed_send.at[to], typed_recv.at[d], typed_ss.at[d], typed_rs.at[d],
            device_id={"mp": to}, device_id_type=MESH)
        copy.start()
        last.append(copy)
    for copy in last:
        copy.wait()
    for t in range(kinds):
        total = typed[m, t]
        for d in range(1, shares):
            total = total + typed_recv[d, t].astype(f32)
        out[t] = jnp.maximum(total, 0.0).T.astype(bf16)


def per_device(features, weights, sample_owner, sample_row, edge_src, edge_dst, edge_count):
    groups, shares = lax.axis_size("dp"), lax.axis_size("mp")
    kinds, feat, rows = features.shape
    sampled, edge_total = sample_row.shape[1], edge_src.shape[1]
    cap = 2 * sampled // groups
    low = min(512, rows, sampled)
    side = groups // HALVES
    width = weights.shape[2] // shares
    bf16, f32, i32 = jnp.bfloat16, jnp.float32, jnp.int32
    vmem = pl.BlockSpec(memory_space=pltpu.VMEM)
    dma = pltpu.SemaphoreType.DMA
    return pl.pallas_call(
        functools.partial(kernel, groups, shares),
        out_shape=jax.ShapeDtypeStruct((kinds, width, SEEDS), bf16),
        in_specs=[vmem] * 7,
        out_specs=vmem,
        scratch_shapes=[
            pltpu.VMEM((STEP, max(sampled, edge_total)), bf16),
            pltpu.VMEM((kinds, rows // low * feat, low), bf16),
            pltpu.VMEM((groups, kinds, cap), i32),
            pltpu.VMEM((groups, kinds, cap), i32),
            pltpu.VMEM((HALVES, kinds, sampled), i32),
            pltpu.VMEM((HALVES, RELS, edge_total), i32),
            pltpu.VMEM((kinds, side, HALVES, feat, cap), bf16),
            pltpu.VMEM((kinds, HALVES, side, feat, cap), bf16),
            pltpu.VMEM((HALVES, RELS, low, sampled // low * SEEDS), bf16),
            pltpu.VMEM((HALVES, RELS, 8, SEEDS), f32),
            pltpu.VMEM((MATS, feat, SEEDS), f32),
            pltpu.VMEM((HALVES, MATS, feat, SEEDS), bf16),
            pltpu.VMEM((HALVES, MATS, feat, SEEDS), bf16),
            pltpu.VMEM((shares, kinds, SEEDS, width), f32),
            pltpu.VMEM((shares, kinds, SEEDS, width), bf16),
            pltpu.VMEM((shares, kinds, SEEDS, width), bf16),
            dma((groups,)), dma((groups,)),
            dma((HALVES, 2)), dma((HALVES, 2)),
            dma((kinds, side, HALVES)), dma((kinds, side, HALVES)),
            dma((HALVES, kinds)), dma((HALVES, kinds)),
            dma((shares,)), dma((shares,)),
        ],
        compiler_params=pltpu.CompilerParams(
            collective_id=0, has_side_effects=True, vmem_limit_bytes=56 * 1024 * 1024),
    )(features, weights, sample_owner[:, :, 0], sample_row, edge_src, edge_dst, edge_count)


def solution(mesh):
    return jax.shard_map(
        per_device,
        mesh=mesh,
        in_specs=(
            P(None, "mp", "dp"),
            P(None, "mp", None),
            P(None, "dp", None),
            P(None, "dp"),
            P(None, "dp"),
            P(None, "dp"),
            P(None, "dp"),
        ),
        out_specs=P(None, "mp", "dp"),
        check_vma=False,
    )
```

```python
import functools

import jax
import jax.numpy as jnp
from jax import lax
from jax.experimental import pallas as pl
from jax.experimental.pallas import tpu as pltpu
from jax.sharding import PartitionSpec as P

SEEDS = 128
RELATION_SOURCE = (0, 1, 0, 1, 2, 0, 2, 1)
MATRIX_TARGET = (1, 0, 0, 2, 1, 2, 0, 1, 0, 1, 2)
RELS = len(RELATION_SOURCE)
KINDS = 3
MATS = RELS + KINDS
SLOTS = tuple(
    tuple([r for r in range(RELS) if RELATION_SOURCE[r] == k] + [RELS + k]) for k in range(KINDS)
)
ORDER = tuple(m for group in SLOTS for m in group)
STARTS = tuple(sum(len(group) for group in SLOTS[:k]) for k in range(KINDS))
RELATIONS = tuple(m for m in ORDER if m < RELS)
HALVES = 2
CORES = 2
STEP = 256
MESH = pl.DeviceIdType.MESH
NT = (((1,), (1,)), ((), ()))
TN = (((0,), (0,)), ((), ()))


def log2(n):
    return n.bit_length() - 1


def kernel(groups, shares, features_in, weights_in, owner, row, src, dst, count, out,
           features, weights, in_sem, iota, tab, req_send, req_recv, pos, edges, send, recv, adj, deg, part,
           part_send, part_recv, typed, typed_send, typed_recv,
           req_ss, req_rs, idx_ss, idx_rs, row_ss, row_rs, part_ss, part_rs, typed_ss, typed_rs, adj_ss, adj_rs):
    kinds, feat, rows = features.shape
    sampled = row.shape[1]
    edge_total = src.shape[1]
    cap = req_send.shape[2]
    low = tab.shape[2]
    share = RELS // CORES
    high = rows // low
    s_high = sampled // low
    side = groups // HALVES
    g = lax.axis_index("dp")
    m = lax.axis_index("mp")
    half = g // side
    q = lax.rem(g, side)
    core = lax.rem(m, CORES)
    f32, bf16, i32 = jnp.float32, jnp.bfloat16, jnp.int32

    def one_hot(index, size):
        n = index.shape[1]
        pieces = []
        for base in range(0, size, STEP):
            span = min(STEP, size - base)
            local = index - base
            local = jnp.where((local >= 0) & (local < span), local, -1).astype(f32).astype(bf16)
            hit = iota[:span, :n] == local
            pieces.append(jnp.where(hit, jnp.ones((), bf16), jnp.zeros((), bf16)))
        return pieces[0] if len(pieces) == 1 else jnp.concatenate(pieces, axis=0)

    load_features = pltpu.make_async_copy(features_in, features, in_sem.at[0])
    load_weights = pltpu.make_async_copy(weights_in, weights, in_sem.at[1])
    load_features.start()
    load_weights.start()
    barrier = pltpu.get_barrier_semaphore()
    for d in range(1, groups):
        pl.semaphore_signal(barrier, inc=1, device_id={"dp": lax.rem(g + d, groups)}, device_id_type=MESH)
    for d in range(1, shares):
        pl.semaphore_signal(barrier, inc=1, device_id={"mp": lax.rem(m + d, shares)}, device_id_type=MESH)

    iota[...] = lax.broadcasted_iota(i32, iota.shape, 0).astype(f32).astype(bf16)
    tri = (lax.broadcasted_iota(i32, (STEP, STEP), 0) <= lax.broadcasted_iota(i32, (STEP, STEP), 1))
    tri = jnp.where(tri, 1.0, 0.0).astype(bf16)
    hot = jnp.concatenate([
        jnp.where(lax.broadcasted_iota(i32, (groups, sampled), 0) == owner[k], 1.0, 0.0)
        for k in range(kinds)], axis=0)
    lines = kinds * groups
    pieces = [hot[:, base:base + STEP] for base in range(0, sampled, STEP)]
    upto = jnp.dot(jnp.concatenate(pieces, axis=0).astype(bf16), tri, preferred_element_type=f32)
    carry = jnp.zeros((lines, 1), f32)
    ranks = []
    for n, piece in enumerate(pieces):
        here = upto[n * lines:(n + 1) * lines]
        ranks.append((here + (carry - 1.0)) * piece)
        carry = carry + here[:, STEP - 1:]
    ranks = jnp.concatenate(ranks, axis=1)
    for k in range(kinds):
        owners = owner[k]
        mine = hot[k * groups:(k + 1) * groups]
        rank = jnp.sum(ranks[k * groups:(k + 1) * groups], axis=0, keepdims=True).astype(i32)
        pos[half, k:k + 1, :] = owners * cap + rank
        wanted = row[k:k + 1, :]
        coarse = mine * (wanted >> 8).astype(f32)
        fine = mine * (wanted & 255).astype(f32)
        pair = jnp.concatenate([coarse, fine], axis=0).astype(bf16)
        listed = lax.dot_general(pair, one_hot(rank, cap), NT, preferred_element_type=f32)
        listed = (listed[:groups] * 256.0 + listed[groups:]).astype(i32)
        for o in range(groups):
            req_send[o, k:k + 1, :] = listed[o:o + 1]
    slots = lax.broadcasted_iota(i32, (1, edge_total), 1)
    for n, r in enumerate(RELATIONS):
        edges[half, n:n + 1, :] = jnp.where(
            slots < count[0, r], dst[r:r + 1, :] * sampled + src[r:r + 1, :], -1)

    pl.semaphore_wait(barrier, groups - 1 + shares - 1)
    asks = []
    for d in range(1, groups):
        to = lax.rem(g + d, groups)
        copy = pltpu.make_async_remote_copy(
            req_send.at[to], req_recv.at[g], req_ss.at[d], req_rs.at[d],
            device_id={"dp": to}, device_id_type=MESH)
        copy.start()
        asks.append(copy)
    hints = []
    for i in range(1, HALVES):
        to = lax.rem(half + i, HALVES) * side + q
        for n, ref in enumerate((pos, edges)):
            copy = pltpu.make_async_remote_copy(
                ref.at[half], ref.at[half], idx_ss.at[i, n], idx_rs.at[i, n],
                device_id={"dp": to}, device_id_type=MESH)
            copy.start()
            hints.append(copy)

    load_features.wait()
    for k in range(kinds):
        for h in range(high):
            tab[k, h * feat:(h + 1) * feat, :] = features[k, :, h * low:(h + 1) * low]

    def build(i, lo_r, hi_r):
        block = lax.rem(half + i, HALVES)

        def one(r, _):
            packed = edges[block, pl.ds(r, 1), :]
            live = packed >= 0
            source = packed & (sampled - 1)
            left = one_hot(jnp.where(live, source & (low - 1), -1), low)
            column = (source >> log2(low)) * SEEDS + (packed >> log2(sampled))
            right = one_hot(jnp.where(live, column, -1), s_high * SEEDS)
            counts = lax.dot_general(left, right, NT, preferred_element_type=f32)
            for h in range(s_high):
                adj[i, r, h * low:(h + 1) * low, :] = counts[:, h * SEEDS:(h + 1) * SEEDS].astype(bf16)
            total = jnp.sum(counts, axis=0, keepdims=True)
            seen = total[:, :SEEDS]
            for h in range(1, s_high):
                seen = seen + total[:, h * SEEDS:(h + 1) * SEEDS]
            deg[i, r] = jnp.broadcast_to(jnp.maximum(seen, 1.0), (8, SEEDS))
            return 0

        lax.fori_loop(core * share + lo_r, core * share + hi_r, one, 0)

    def share_block(i):
        built = pl.ds(core * share, share)
        copies = []
        for n, ref in enumerate((adj, deg)):
            copies.append(pltpu.make_async_remote_copy(
                ref.at[i, built], ref.at[i, built], adj_ss.at[i, n], adj_rs.at[i, n],
                device_id={"mp": m - core + lax.rem(core + 1, CORES)}, device_id_type=MESH))
            copies[-1].start()
        return copies

    build(0, 0, 1)
    req_recv[g] = req_send[g]
    for copy in asks:
        copy.wait()

    def pick(k, block):
        wanted = req_recv[block, k:k + 1, :]
        found = jnp.dot(tab[k], one_hot(wanted & (low - 1), low), preferred_element_type=f32)
        bank = wanted >> log2(low)
        chosen = jnp.zeros((feat, cap), f32)
        for h in range(high):
            chosen = jnp.where(bank == h, found[h * feat:(h + 1) * feat], chosen)
        return chosen.astype(bf16)

    def row_copy(k, d, j):
        return pltpu.make_async_remote_copy(
            send.at[k, d, j], recv.at[k, j, q], row_ss.at[k, d, j], row_rs.at[k, d, j],
            device_id={"dp": half * side + lax.rem(q + d, side)}, device_id_type=MESH)

    for k in range(kinds):
        def serve(n, _, k=k):
            d, j = 1 + lax.rem(n, side - 1), lax.rem(half + 1 + n // (side - 1), HALVES)
            send[k, d, j] = pick(k, j * side + lax.rem(q + d, side))
            row_copy(k, d, j).start()
            return 0

        lax.fori_loop(0, (side - 1) * HALVES, serve, 0)
    for k in range(kinds):
        def keep(j, _, k=k):
            recv[k, j, q] = pick(k, j * side + q)
            return 0

        lax.fori_loop(0, HALVES, keep, 0)

    build(0, 1, share)
    shared = share_block(0)
    for copy in hints:
        copy.wait()
    for i in range(1, HALVES):
        build(i, 0, share)
        shared += share_block(i)
    for copy in shared:
        copy.wait()

    replies = [[] for _ in range(kinds)]
    sums = [None] * kinds

    def finish(k):
        for copy in replies[k]:
            copy.wait()
        for n, matrix in enumerate(SLOTS[k]):
            message = part[STARTS[k] + n]
            for i in range(1, HALVES):
                message = message + part_recv[i, STARTS[k] + n].astype(f32)
            term = lax.dot_general(message.astype(bf16), weights[matrix], TN, preferred_element_type=f32)
            t = MATRIX_TARGET[matrix]
            sums[t] = term if sums[t] is None else sums[t] + term

    for k in range(kinds):
        start, size = STARTS[k], len(SLOTS[k])
        first = start - k
        for i in reversed(range(HALVES)):
            block = lax.rem(half + i, HALVES)

            def landed(n, _, k=k, block=block):
                row_copy(k, 1 + n, block).wait()
                return 0

            lax.fori_loop(0, side - 1, landed, 0)
            stack = recv[k, block].reshape(side * feat, cap)
            gathered = []
            for h in range(s_high):
                where = pos[block, k:k + 1, h * low:(h + 1) * low]
                found = jnp.dot(stack, one_hot(where & (cap - 1), cap), preferred_element_type=f32)
                holder = (where >> log2(cap)) - half * side
                chosen = jnp.zeros((feat, low), f32)
                for o in range(side):
                    chosen = jnp.where(holder == o, found[o * feat:(o + 1) * feat], chosen)
                gathered.append(chosen.astype(bf16))
            gathered = jnp.concatenate(gathered, axis=1)
            counts = jnp.concatenate([adj[i, first + n] for n in range(size - 1)], axis=1)
            summed = jnp.dot(gathered, counts, preferred_element_type=f32)
            values = [summed[:, n * SEEDS:(n + 1) * SEEDS] / deg[i, first + n][:1] for n in range(size - 1)]
            values.append(gathered[:, :SEEDS].astype(f32))
            for n, value in enumerate(values):
                if i == 0:
                    part[start + n] = value
                else:
                    part_send[i, start + n] = value.astype(bf16)
            if i > 0:
                copy = pltpu.make_async_remote_copy(
                    part_send.at[i, pl.ds(start, size)], part_recv.at[i, pl.ds(start, size)],
                    part_ss.at[i, k], part_rs.at[i, k],
                    device_id={"dp": block * side + q}, device_id_type=MESH)
                copy.start()
                replies[k].append(copy)
        if k == 0:
            load_weights.wait()
        else:
            finish(k - 1)
    finish(kinds - 1)
    width = typed.shape[3]
    for t in range(kinds):
        for p in range(shares):
            piece = sums[t][:, p * width:(p + 1) * width]
            typed[p, t] = piece
            typed_send[p, t] = piece.astype(bf16)
    last = []
    for d in range(1, shares):
        to = lax.rem(m + d, shares)
        copy = pltpu.make_async_remote_copy(
            typed_send.at[to], typed_recv.at[d], typed_ss.at[d], typed_rs.at[d],
            device_id={"mp": to}, device_id_type=MESH)
        copy.start()
        last.append(copy)
    for copy in last:
        copy.wait()
    for t in range(kinds):
        total = typed[m, t]
        for d in range(1, shares):
            total = total + typed_recv[d, t].astype(f32)
        out[t] = jnp.maximum(total, 0.0).T.astype(bf16)


def per_device(features, weights, sample_owner, sample_row, edge_src, edge_dst, edge_count):
    groups, shares = lax.axis_size("dp"), lax.axis_size("mp")
    kinds, feat, rows = features.shape
    sampled, edge_total = sample_row.shape[1], edge_src.shape[1]
    cap = 2 * sampled // groups
    low = min(512, rows, sampled)
    side = groups // HALVES
    width = weights.shape[2] // shares
    bf16, f32, i32 = jnp.bfloat16, jnp.float32, jnp.int32
    vmem = pl.BlockSpec(memory_space=pltpu.VMEM)
    any_space = pl.BlockSpec(memory_space=pl.ANY)
    dma = pltpu.SemaphoreType.DMA
    return pl.pallas_call(
        functools.partial(kernel, groups, shares),
        out_shape=jax.ShapeDtypeStruct((kinds, width, SEEDS), bf16),
        in_specs=[any_space] * 2 + [vmem] * 4 + [pl.BlockSpec(memory_space=pltpu.SMEM)],
        out_specs=vmem,
        scratch_shapes=[
            pltpu.VMEM(features.shape, bf16),
            pltpu.VMEM(weights.shape, bf16),
            dma((2,)),
            pltpu.VMEM((STEP, max(sampled, edge_total)), bf16),
            pltpu.VMEM((kinds, rows // low * feat, low), bf16),
            pltpu.VMEM((groups, kinds, cap), i32),
            pltpu.VMEM((groups, kinds, cap), i32),
            pltpu.VMEM((HALVES, kinds, sampled), i32),
            pltpu.VMEM((HALVES, RELS, edge_total), i32),
            pltpu.VMEM((kinds, side, HALVES, feat, cap), bf16),
            pltpu.VMEM((kinds, HALVES, side, feat, cap), bf16),
            pltpu.VMEM((HALVES, RELS, sampled, SEEDS), bf16),
            pltpu.VMEM((HALVES, RELS, 8, SEEDS), f32),
            pltpu.VMEM((MATS, feat, SEEDS), f32),
            pltpu.VMEM((HALVES, MATS, feat, SEEDS), bf16),
            pltpu.VMEM((HALVES, MATS, feat, SEEDS), bf16),
            pltpu.VMEM((shares, kinds, SEEDS, width), f32),
            pltpu.VMEM((shares, kinds, SEEDS, width), bf16),
            pltpu.VMEM((shares, kinds, SEEDS, width), bf16),
            dma((groups,)), dma((groups,)),
            dma((HALVES, 2)), dma((HALVES, 2)),
            dma((kinds, side, HALVES)), dma((kinds, side, HALVES)),
            dma((HALVES, kinds)), dma((HALVES, kinds)),
            dma((shares,)), dma((shares,)),
            dma((HALVES, 2)), dma((HALVES, 2)),
        ],
        compiler_params=pltpu.CompilerParams(
            collective_id=0, has_side_effects=True, vmem_limit_bytes=56 * 1024 * 1024),
    )(features, weights, sample_owner.transpose(0, 2, 1), sample_row, edge_src, edge_dst, edge_count.T)


def solution(mesh):
    return jax.shard_map(
        per_device,
        mesh=mesh,
        in_specs=(
            P(None, "mp", "dp"),
            P(None, "mp", None),
            P(None, "dp", None),
            P(None, "dp"),
            P(None, "dp"),
            P(None, "dp"),
            P(None, "dp"),
        ),
        out_specs=P(None, "mp", "dp"),
        check_vma=False,
    )
```

```python
import functools

import jax
import jax.numpy as jnp
from jax import lax
from jax.experimental import pallas as pl
from jax.experimental.pallas import tpu as pltpu
from jax.sharding import PartitionSpec as P

SEEDS = 128
RELATION_SOURCE = (0, 1, 0, 1, 2, 0, 2, 1)
MATRIX_TARGET = (1, 0, 0, 2, 1, 2, 0, 1, 0, 1, 2)
RELS = len(RELATION_SOURCE)
KINDS = 3
MATS = RELS + KINDS
SLOTS = tuple(
    tuple([r for r in range(RELS) if RELATION_SOURCE[r] == k] + [RELS + k]) for k in range(KINDS)
)
ORDER = tuple(m for group in SLOTS for m in group)
STARTS = tuple(sum(len(group) for group in SLOTS[:k]) for k in range(KINDS))
RELATIONS = tuple(m for m in ORDER if m < RELS)
HALVES = 2
CORES = 2
STEP = 256
MESH = pl.DeviceIdType.MESH
NT = (((1,), (1,)), ((), ()))
TN = (((0,), (0,)), ((), ()))


def log2(n):
    return n.bit_length() - 1


def kernel(groups, shares, features_in, weights_in, owner, row, src, dst, count, out,
           features, weights, in_sem, iota, tab, req_send, req_recv, pos, edges, send, recv, adj, deg, part,
           part_send, part_recv, typed, typed_send, typed_recv,
           req_ss, req_rs, idx_ss, idx_rs, row_ss, row_rs, part_ss, part_rs, typed_ss, typed_rs, adj_ss, adj_rs):
    kinds, feat, rows = features.shape
    sampled = row.shape[1]
    edge_total = src.shape[1]
    cap = req_send.shape[2]
    low = tab.shape[2]
    share = RELS // CORES
    high = rows // low
    s_high = sampled // low
    side = groups // HALVES
    g = lax.axis_index("dp")
    m = lax.axis_index("mp")
    half = g // side
    q = lax.rem(g, side)
    core = lax.rem(m, CORES)
    f32, bf16, i32 = jnp.float32, jnp.bfloat16, jnp.int32

    def one_hot(index, size):
        n = index.shape[1]
        pieces = []
        for base in range(0, size, STEP):
            span = min(STEP, size - base)
            local = index - base
            local = jnp.where((local >= 0) & (local < span), local, -1).astype(f32).astype(bf16)
            hit = iota[:span, :n] == local
            pieces.append(jnp.where(hit, jnp.ones((), bf16), jnp.zeros((), bf16)))
        return pieces[0] if len(pieces) == 1 else jnp.concatenate(pieces, axis=0)

    load_features = pltpu.make_async_copy(features_in, features, in_sem.at[0])
    load_weights = pltpu.make_async_copy(weights_in, weights, in_sem.at[1])
    load_features.start()
    load_weights.start()
    barrier = pltpu.get_barrier_semaphore()
    for d in range(1, groups):
        pl.semaphore_signal(barrier, inc=1, device_id={"dp": lax.rem(g + d, groups)}, device_id_type=MESH)
    for d in range(1, shares):
        pl.semaphore_signal(barrier, inc=1, device_id={"mp": lax.rem(m + d, shares)}, device_id_type=MESH)

    iota[...] = lax.broadcasted_iota(i32, iota.shape, 0).astype(f32).astype(bf16)
    tri = (lax.broadcasted_iota(i32, (STEP, STEP), 0) <= lax.broadcasted_iota(i32, (STEP, STEP), 1))
    tri = jnp.where(tri, 1.0, 0.0).astype(bf16)
    hot = jnp.concatenate([
        jnp.where(lax.broadcasted_iota(i32, (groups, sampled), 0) == owner[k], 1.0, 0.0)
        for k in range(kinds)], axis=0)
    lines = kinds * groups
    pieces = [hot[:, base:base + STEP] for base in range(0, sampled, STEP)]
    upto = jnp.dot(jnp.concatenate(pieces, axis=0).astype(bf16), tri, preferred_element_type=f32)
    carry = jnp.zeros((lines, 1), f32)
    ranks = []
    for n, piece in enumerate(pieces):
        here = upto[n * lines:(n + 1) * lines]
        ranks.append((here + (carry - 1.0)) * piece)
        carry = carry + here[:, STEP - 1:]
    ranks = jnp.concatenate(ranks, axis=1)
    for k in range(kinds):
        owners = owner[k]
        mine = hot[k * groups:(k + 1) * groups]
        rank = jnp.sum(ranks[k * groups:(k + 1) * groups], axis=0, keepdims=True).astype(i32)
        pos[half, k:k + 1, :] = owners * cap + rank
        wanted = row[k:k + 1, :]
        coarse = mine * (wanted >> 8).astype(f32)
        fine = mine * (wanted & 255).astype(f32)
        pair = jnp.concatenate([coarse, fine], axis=0).astype(bf16)
        listed = lax.dot_general(pair, one_hot(rank, cap), NT, preferred_element_type=f32)
        listed = (listed[:groups] * 256.0 + listed[groups:]).astype(i32)
        for o in range(groups):
            req_send[o, k:k + 1, :] = listed[o:o + 1]
    slots = lax.broadcasted_iota(i32, (1, edge_total), 1)
    for n, r in enumerate(RELATIONS):
        edges[half, n:n + 1, :] = jnp.where(
            slots < count[0, r], dst[r:r + 1, :] * sampled + src[r:r + 1, :], -1)

    pl.semaphore_wait(barrier, groups - 1 + shares - 1)
    asks = []
    for d in range(1, groups):
        to = lax.rem(g + d, groups)
        copy = pltpu.make_async_remote_copy(
            req_send.at[to], req_recv.at[g], req_ss.at[d], req_rs.at[d],
            device_id={"dp": to}, device_id_type=MESH)
        copy.start()
        asks.append(copy)
    load_features.wait()
    for k in range(kinds):
        for h in range(high):
            tab[k, h * feat:(h + 1) * feat, :] = features[k, :, h * low:(h + 1) * low]

    def unit_copy(i, r, n):
        ref = (adj, deg)[n]
        return pltpu.make_async_remote_copy(
            ref.at[i, r], ref.at[i, r], adj_ss.at[i, lax.rem(r, share), n], adj_rs.at[i, lax.rem(r, share), n],
            device_id={"mp": m - core + lax.rem(core + 1, CORES)}, device_id_type=MESH)

    def build(i, lo_r, hi_r):
        block = lax.rem(half + i, HALVES)

        def one(r, _):
            packed = edges[block, pl.ds(r, 1), :]
            live = packed >= 0
            source = packed & (sampled - 1)
            left = one_hot(jnp.where(live, source & (low - 1), -1), low)
            column = (source >> log2(low)) * SEEDS + (packed >> log2(sampled))
            right = one_hot(jnp.where(live, column, -1), s_high * SEEDS)
            counts = lax.dot_general(left, right, NT, preferred_element_type=f32)
            for h in range(s_high):
                adj[i, r, h * low:(h + 1) * low, :] = counts[:, h * SEEDS:(h + 1) * SEEDS].astype(bf16)
            total = jnp.sum(counts, axis=0, keepdims=True)
            seen = total[:, :SEEDS]
            for h in range(1, s_high):
                seen = seen + total[:, h * SEEDS:(h + 1) * SEEDS]
            deg[i, r] = jnp.broadcast_to(jnp.maximum(seen, 1.0), (8, SEEDS))
            for n in range(2):
                unit_copy(i, r, n).start()
            return 0

        lax.fori_loop(core * share + lo_r, core * share + hi_r, one, 0)

    build(0, 0, 1)
    req_recv[g] = req_send[g]
    for copy in asks:
        copy.wait()
    hints = []
    for i in range(1, HALVES):
        to = lax.rem(half + i, HALVES) * side + q
        for n, ref in enumerate((pos, edges)):
            copy = pltpu.make_async_remote_copy(
                ref.at[half], ref.at[half], idx_ss.at[i, n], idx_rs.at[i, n],
                device_id={"dp": to}, device_id_type=MESH)
            copy.start()
            hints.append(copy)


    def pick(k, block):
        wanted = req_recv[block, k:k + 1, :]
        found = jnp.dot(tab[k], one_hot(wanted & (low - 1), low), preferred_element_type=f32)
        bank = wanted >> log2(low)
        chosen = jnp.zeros((feat, cap), f32)
        for h in range(high):
            chosen = jnp.where(bank == h, found[h * feat:(h + 1) * feat], chosen)
        return chosen.astype(bf16)

    def row_copy(k, d, j):
        return pltpu.make_async_remote_copy(
            send.at[k, d, j], recv.at[k, j, q], row_ss.at[k, d, j], row_rs.at[k, d, j],
            device_id={"dp": half * side + lax.rem(q + d, side)}, device_id_type=MESH)

    for k in range(kinds):
        def serve(n, _, k=k):
            d, j = 1 + lax.rem(n, side - 1), lax.rem(half + 1 + n // (side - 1), HALVES)
            send[k, d, j] = pick(k, j * side + lax.rem(q + d, side))
            row_copy(k, d, j).start()
            return 0

        lax.fori_loop(0, (side - 1) * HALVES, serve, 0)
    for k in range(kinds):
        def keep(j, _, k=k):
            recv[k, j, q] = pick(k, j * side + q)
            return 0

        lax.fori_loop(0, HALVES, keep, 0)

    build(0, 1, share)
    for copy in hints:
        copy.wait()
    for i in range(1, HALVES):
        build(i, 0, share)

    def arrived(r, _):
        for i in range(HALVES):
            for n in range(2):
                unit_copy(i, core * share + r, n).wait()
        return 0

    lax.fori_loop(0, share, arrived, 0)

    replies = [[] for _ in range(kinds)]
    sums = [None] * kinds

    def finish(k):
        for copy in replies[k]:
            copy.wait()
        for n, matrix in enumerate(SLOTS[k]):
            message = part[STARTS[k] + n]
            for i in range(1, HALVES):
                message = message + part_recv[i, STARTS[k] + n].astype(f32)
            term = lax.dot_general(message.astype(bf16), weights[matrix], TN, preferred_element_type=f32)
            t = MATRIX_TARGET[matrix]
            sums[t] = term if sums[t] is None else sums[t] + term

    for k in range(kinds):
        start, size = STARTS[k], len(SLOTS[k])
        first = start - k
        for i in reversed(range(HALVES)):
            block = lax.rem(half + i, HALVES)

            def landed(n, _, k=k, block=block):
                row_copy(k, 1 + n, block).wait()
                return 0

            lax.fori_loop(0, side - 1, landed, 0)
            stack = recv[k, block].reshape(side * feat, cap)
            gathered = []
            for h in range(s_high):
                where = pos[block, k:k + 1, h * low:(h + 1) * low]
                found = jnp.dot(stack, one_hot(where & (cap - 1), cap), preferred_element_type=f32)
                holder = (where >> log2(cap)) - half * side
                chosen = jnp.zeros((feat, low), f32)
                for o in range(side):
                    chosen = jnp.where(holder == o, found[o * feat:(o + 1) * feat], chosen)
                gathered.append(chosen.astype(bf16))
            gathered = jnp.concatenate(gathered, axis=1)
            counts = jnp.concatenate([adj[i, first + n] for n in range(size - 1)], axis=1)
            summed = jnp.dot(gathered, counts, preferred_element_type=f32)
            values = [summed[:, n * SEEDS:(n + 1) * SEEDS] / deg[i, first + n][:1] for n in range(size - 1)]
            values.append(gathered[:, :SEEDS].astype(f32))
            for n, value in enumerate(values):
                if i == 0:
                    part[start + n] = value
                else:
                    part_send[i, start + n] = value.astype(bf16)
            if i > 0:
                copy = pltpu.make_async_remote_copy(
                    part_send.at[i, pl.ds(start, size)], part_recv.at[i, pl.ds(start, size)],
                    part_ss.at[i, k], part_rs.at[i, k],
                    device_id={"dp": block * side + q}, device_id_type=MESH)
                copy.start()
                replies[k].append(copy)
        if k == 0:
            load_weights.wait()
        else:
            finish(k - 1)
    finish(kinds - 1)
    width = typed.shape[3]
    for t in range(kinds):
        for p in range(shares):
            piece = sums[t][:, p * width:(p + 1) * width]
            typed[p, t] = piece
            typed_send[p, t] = piece.astype(bf16)
    last = []
    for d in range(1, shares):
        to = lax.rem(m + d, shares)
        copy = pltpu.make_async_remote_copy(
            typed_send.at[to], typed_recv.at[d], typed_ss.at[d], typed_rs.at[d],
            device_id={"mp": to}, device_id_type=MESH)
        copy.start()
        last.append(copy)
    for copy in last:
        copy.wait()
    for t in range(kinds):
        total = typed[m, t]
        for d in range(1, shares):
            total = total + typed_recv[d, t].astype(f32)
        out[t] = jnp.maximum(total, 0.0).T.astype(bf16)


def per_device(features, weights, sample_owner, sample_row, edge_src, edge_dst, edge_count):
    groups, shares = lax.axis_size("dp"), lax.axis_size("mp")
    kinds, feat, rows = features.shape
    sampled, edge_total = sample_row.shape[1], edge_src.shape[1]
    cap = 2 * sampled // groups
    low = min(512, rows, sampled)
    side = groups // HALVES
    width = weights.shape[2] // shares
    bf16, f32, i32 = jnp.bfloat16, jnp.float32, jnp.int32
    vmem = pl.BlockSpec(memory_space=pltpu.VMEM)
    any_space = pl.BlockSpec(memory_space=pl.ANY)
    dma = pltpu.SemaphoreType.DMA
    return pl.pallas_call(
        functools.partial(kernel, groups, shares),
        out_shape=jax.ShapeDtypeStruct((kinds, width, SEEDS), bf16),
        in_specs=[any_space] * 2 + [vmem] * 4 + [pl.BlockSpec(memory_space=pltpu.SMEM)],
        out_specs=vmem,
        scratch_shapes=[
            pltpu.VMEM(features.shape, bf16),
            pltpu.VMEM(weights.shape, bf16),
            dma((2,)),
            pltpu.VMEM((STEP, max(sampled, edge_total)), bf16),
            pltpu.VMEM((kinds, rows // low * feat, low), bf16),
            pltpu.VMEM((groups, kinds, cap), i32),
            pltpu.VMEM((groups, kinds, cap), i32),
            pltpu.VMEM((HALVES, kinds, sampled), i32),
            pltpu.VMEM((HALVES, RELS, edge_total), i32),
            pltpu.VMEM((kinds, side, HALVES, feat, cap), bf16),
            pltpu.VMEM((kinds, HALVES, side, feat, cap), bf16),
            pltpu.VMEM((HALVES, RELS, sampled, SEEDS), bf16),
            pltpu.VMEM((HALVES, RELS, 8, SEEDS), f32),
            pltpu.VMEM((MATS, feat, SEEDS), f32),
            pltpu.VMEM((HALVES, MATS, feat, SEEDS), bf16),
            pltpu.VMEM((HALVES, MATS, feat, SEEDS), bf16),
            pltpu.VMEM((shares, kinds, SEEDS, width), f32),
            pltpu.VMEM((shares, kinds, SEEDS, width), bf16),
            pltpu.VMEM((shares, kinds, SEEDS, width), bf16),
            dma((groups,)), dma((groups,)),
            dma((HALVES, 2)), dma((HALVES, 2)),
            dma((kinds, side, HALVES)), dma((kinds, side, HALVES)),
            dma((HALVES, kinds)), dma((HALVES, kinds)),
            dma((shares,)), dma((shares,)),
            dma((HALVES, RELS // CORES, 2)), dma((HALVES, RELS // CORES, 2)),
        ],
        compiler_params=pltpu.CompilerParams(
            collective_id=0, has_side_effects=True, vmem_limit_bytes=56 * 1024 * 1024),
    )(features, weights, sample_owner.transpose(0, 2, 1), sample_row, edge_src, edge_dst, edge_count.T)


def solution(mesh):
    return jax.shard_map(
        per_device,
        mesh=mesh,
        in_specs=(
            P(None, "mp", "dp"),
            P(None, "mp", None),
            P(None, "dp", None),
            P(None, "dp"),
            P(None, "dp"),
            P(None, "dp"),
            P(None, "dp"),
        ),
        out_specs=P(None, "mp", "dp"),
        check_vma=False,
    )
```

```python
import functools

import jax
import jax.numpy as jnp
from jax import lax
from jax.experimental import pallas as pl
from jax.experimental.pallas import tpu as pltpu
from jax.sharding import PartitionSpec as P

SEEDS = 128
RELATION_SOURCE = (0, 1, 0, 1, 2, 0, 2, 1)
MATRIX_TARGET = (1, 0, 0, 2, 1, 2, 0, 1, 0, 1, 2)
RELS = len(RELATION_SOURCE)
KINDS = 3
MATS = RELS + KINDS
SLOTS = tuple(
    tuple([r for r in range(RELS) if RELATION_SOURCE[r] == k] + [RELS + k]) for k in range(KINDS)
)
ORDER = tuple(m for group in SLOTS for m in group)
STARTS = tuple(sum(len(group) for group in SLOTS[:k]) for k in range(KINDS))
RELATIONS = tuple(m for m in ORDER if m < RELS)
HALVES = 2
CORES = 2
STEP = 256
MESH = pl.DeviceIdType.MESH
NT = (((1,), (1,)), ((), ()))
TN = (((0,), (0,)), ((), ()))


def log2(n):
    return n.bit_length() - 1


def kernel(groups, shares, features_in, weights_in, owner, row, src, dst, count, out,
           features, weights, in_sem, iota, tab, req_send, req_recv, pos, edges, send, recv, adj, deg, part,
           part_send, part_recv, typed, typed_send, typed_recv,
           req_ss, req_rs, idx_ss, idx_rs, row_ss, row_rs, part_ss, part_rs, typed_ss, typed_rs, adj_ss, adj_rs):
    kinds, feat, rows = features.shape
    sampled = row.shape[1]
    edge_total = src.shape[1]
    cap = req_send.shape[2]
    low = tab.shape[2]
    share = RELS // CORES
    high = rows // low
    s_high = sampled // low
    side = groups // HALVES
    g = lax.axis_index("dp")
    m = lax.axis_index("mp")
    half = g // side
    q = lax.rem(g, side)
    core = lax.rem(m, CORES)
    f32, bf16, i32 = jnp.float32, jnp.bfloat16, jnp.int32

    def one_hot(index, size):
        n = index.shape[1]
        pieces = []
        for base in range(0, size, STEP):
            span = min(STEP, size - base)
            local = index - base
            local = jnp.where((local >= 0) & (local < span), local, -1).astype(f32).astype(bf16)
            hit = iota[:span, :n] == local
            pieces.append(jnp.where(hit, jnp.ones((), bf16), jnp.zeros((), bf16)))
        return pieces[0] if len(pieces) == 1 else jnp.concatenate(pieces, axis=0)

    load_features = pltpu.make_async_copy(features_in, features, in_sem.at[0])
    load_weights = pltpu.make_async_copy(weights_in, weights, in_sem.at[1])
    load_features.start()
    load_weights.start()
    barrier = pltpu.get_barrier_semaphore()
    for d in range(1, groups):
        pl.semaphore_signal(barrier, inc=1, device_id={"dp": lax.rem(g + d, groups)}, device_id_type=MESH)
    for d in range(1, shares):
        pl.semaphore_signal(barrier, inc=1, device_id={"mp": lax.rem(m + d, shares)}, device_id_type=MESH)

    iota[...] = lax.broadcasted_iota(i32, iota.shape, 0).astype(f32).astype(bf16)
    tri = (lax.broadcasted_iota(i32, (STEP, STEP), 0) <= lax.broadcasted_iota(i32, (STEP, STEP), 1))
    tri = jnp.where(tri, 1.0, 0.0).astype(bf16)
    hot = jnp.concatenate([
        jnp.where(lax.broadcasted_iota(i32, (groups, sampled), 0) == owner[k], 1.0, 0.0)
        for k in range(kinds)], axis=0)
    lines = kinds * groups
    pieces = [hot[:, base:base + STEP] for base in range(0, sampled, STEP)]
    upto = jnp.dot(jnp.concatenate(pieces, axis=0).astype(bf16), tri, preferred_element_type=f32)
    carry = jnp.zeros((lines, 1), f32)
    ranks = []
    for n, piece in enumerate(pieces):
        here = upto[n * lines:(n + 1) * lines]
        ranks.append((here + (carry - 1.0)) * piece)
        carry = carry + here[:, STEP - 1:]
    ranks = jnp.concatenate(ranks, axis=1)
    for k in range(kinds):
        owners = owner[k]
        mine = hot[k * groups:(k + 1) * groups]
        rank = jnp.sum(ranks[k * groups:(k + 1) * groups], axis=0, keepdims=True).astype(i32)
        pos[half, k:k + 1, :] = owners * cap + rank
        wanted = row[k:k + 1, :]
        coarse = mine * (wanted >> 8).astype(f32)
        fine = mine * (wanted & 255).astype(f32)
        pair = jnp.concatenate([coarse, fine], axis=0).astype(bf16)
        listed = lax.dot_general(pair, one_hot(rank, cap), NT, preferred_element_type=f32)
        listed = (listed[:groups] * 256.0 + listed[groups:]).astype(i32)
        for o in range(groups):
            req_send[o, k:k + 1, :] = listed[o:o + 1]
    slots = lax.broadcasted_iota(i32, (1, edge_total), 1)
    for n, r in enumerate(RELATIONS):
        edges[half, n:n + 1, :] = jnp.where(
            slots < count[0, r], dst[r:r + 1, :] * sampled + src[r:r + 1, :], -1)

    pl.semaphore_wait(barrier, groups - 1 + shares - 1)
    asks = []
    for d in range(1, groups):
        to = lax.rem(g + d, groups)
        copy = pltpu.make_async_remote_copy(
            req_send.at[to], req_recv.at[g], req_ss.at[d], req_rs.at[d],
            device_id={"dp": to}, device_id_type=MESH)
        copy.start()
        asks.append(copy)
    hints = []
    for i in range(1, HALVES):
        to = lax.rem(half + i, HALVES) * side + q
        for n, ref in enumerate((pos, edges)):
            copy = pltpu.make_async_remote_copy(
                ref.at[half], ref.at[half], idx_ss.at[i, n], idx_rs.at[i, n],
                device_id={"dp": to}, device_id_type=MESH)
            copy.start()
            hints.append(copy)

    load_features.wait()
    for k in range(kinds):
        for h in range(high):
            tab[k, h * feat:(h + 1) * feat, :] = features[k, :, h * low:(h + 1) * low]

    def unit_copy(i, r, n):
        ref = (adj, deg)[n]
        return pltpu.make_async_remote_copy(
            ref.at[i, r], ref.at[i, r], adj_ss.at[i, lax.rem(r, share), n], adj_rs.at[i, lax.rem(r, share), n],
            device_id={"mp": m - core + lax.rem(core + 1, CORES)}, device_id_type=MESH)

    def build(i, lo_r, hi_r):
        block = lax.rem(half + i, HALVES)

        def one(r, _):
            packed = edges[block, pl.ds(r, 1), :]
            live = packed >= 0
            source = packed & (sampled - 1)
            left = one_hot(jnp.where(live, source & (low - 1), -1), low)
            column = (source >> log2(low)) * SEEDS + (packed >> log2(sampled))
            right = one_hot(jnp.where(live, column, -1), s_high * SEEDS)
            counts = lax.dot_general(left, right, NT, preferred_element_type=f32)
            for h in range(s_high):
                adj[i, r, h * low:(h + 1) * low, :] = counts[:, h * SEEDS:(h + 1) * SEEDS].astype(bf16)
            total = jnp.sum(counts, axis=0, keepdims=True)
            seen = total[:, :SEEDS]
            for h in range(1, s_high):
                seen = seen + total[:, h * SEEDS:(h + 1) * SEEDS]
            deg[i, r] = jnp.broadcast_to(jnp.maximum(seen, 1.0), (8, SEEDS))
            for n in range(2):
                unit_copy(i, r, n).start()
            return 0

        lax.fori_loop(core * share + lo_r, core * share + hi_r, one, 0)

    build(0, 0, 1)
    req_recv[g] = req_send[g]
    for copy in asks:
        copy.wait()

    def pick(k, block):
        wanted = req_recv[block, k:k + 1, :]
        found = jnp.dot(tab[k], one_hot(wanted & (low - 1), low), preferred_element_type=f32)
        bank = wanted >> log2(low)
        chosen = jnp.zeros((feat, cap), f32)
        for h in range(high):
            chosen = jnp.where(bank == h, found[h * feat:(h + 1) * feat], chosen)
        return chosen.astype(bf16)

    def row_copy(k, d, j):
        return pltpu.make_async_remote_copy(
            send.at[k, d, j], recv.at[k, j, q], row_ss.at[k, d, j], row_rs.at[k, d, j],
            device_id={"dp": half * side + lax.rem(q + d, side)}, device_id_type=MESH)

    for k in range(kinds):
        def serve(n, _, k=k):
            d, j = 1 + lax.rem(n, side - 1), lax.rem(half + 1 + n // (side - 1), HALVES)
            send[k, d, j] = pick(k, j * side + lax.rem(q + d, side))
            row_copy(k, d, j).start()
            return 0

        lax.fori_loop(0, (side - 1) * HALVES, serve, 0)
    for k in range(kinds):
        def keep(j, _, k=k):
            recv[k, j, q] = pick(k, j * side + q)
            return 0

        lax.fori_loop(0, HALVES, keep, 0)

    build(0, 1, share)
    for copy in hints:
        copy.wait()
    for i in range(1, HALVES):
        build(i, 0, share)

    def arrived(r, _):
        for i in range(HALVES):
            for n in range(2):
                unit_copy(i, core * share + r, n).wait()
        return 0

    lax.fori_loop(0, share, arrived, 0)

    replies = [[] for _ in range(kinds)]
    sums = [None] * kinds

    def finish(k):
        for copy in replies[k]:
            copy.wait()
        for n, matrix in enumerate(SLOTS[k]):
            message = part[STARTS[k] + n]
            for i in range(1, HALVES):
                message = message + part_recv[i, STARTS[k] + n].astype(f32)
            term = lax.dot_general(message.astype(bf16), weights[matrix], TN, preferred_element_type=f32)
            t = MATRIX_TARGET[matrix]
            sums[t] = term if sums[t] is None else sums[t] + term

    for k in range(kinds):
        start, size = STARTS[k], len(SLOTS[k])
        first = start - k
        for i in reversed(range(HALVES)):
            block = lax.rem(half + i, HALVES)

            def landed(n, _, k=k, block=block):
                row_copy(k, 1 + n, block).wait()
                return 0

            lax.fori_loop(0, side - 1, landed, 0)
            stack = recv[k, block].reshape(side * feat, cap)
            gathered = []
            for h in range(s_high):
                where = pos[block, k:k + 1, h * low:(h + 1) * low]
                found = jnp.dot(stack, one_hot(where & (cap - 1), cap), preferred_element_type=f32)
                holder = (where >> log2(cap)) - half * side
                chosen = jnp.zeros((feat, low), f32)
                for o in range(side):
                    chosen = jnp.where(holder == o, found[o * feat:(o + 1) * feat], chosen)
                gathered.append(chosen.astype(bf16))
            gathered = jnp.concatenate(gathered, axis=1)
            counts = jnp.concatenate([adj[i, first + n] for n in range(size - 1)], axis=1)
            summed = jnp.dot(gathered, counts, preferred_element_type=f32)
            values = [summed[:, n * SEEDS:(n + 1) * SEEDS] / deg[i, first + n][:1] for n in range(size - 1)]
            values.append(gathered[:, :SEEDS].astype(f32))
            for n, value in enumerate(values):
                if i == 0:
                    part[start + n] = value
                else:
                    part_send[i, start + n] = value.astype(bf16)
            if i > 0:
                copy = pltpu.make_async_remote_copy(
                    part_send.at[i, pl.ds(start, size)], part_recv.at[i, pl.ds(start, size)],
                    part_ss.at[i, k], part_rs.at[i, k],
                    device_id={"dp": block * side + q}, device_id_type=MESH)
                copy.start()
                replies[k].append(copy)
        if k == 0:
            load_weights.wait()
        else:
            finish(k - 1)
    finish(kinds - 1)
    width = typed.shape[3]
    for t in range(kinds):
        for p in range(shares):
            piece = sums[t][:, p * width:(p + 1) * width]
            typed[p, t] = piece
            typed_send[p, t] = piece.astype(bf16)
    last = []
    for d in range(1, shares):
        to = lax.rem(m + d, shares)
        copy = pltpu.make_async_remote_copy(
            typed_send.at[to], typed_recv.at[d], typed_ss.at[d], typed_rs.at[d],
            device_id={"mp": to}, device_id_type=MESH)
        copy.start()
        last.append(copy)
    for copy in last:
        copy.wait()
    for t in range(kinds):
        total = typed[m, t]
        for d in range(1, shares):
            total = total + typed_recv[d, t].astype(f32)
        out[t] = jnp.maximum(total, 0.0).T.astype(bf16)


def per_device(features, weights, sample_owner, sample_row, edge_src, edge_dst, edge_count):
    groups, shares = lax.axis_size("dp"), lax.axis_size("mp")
    kinds, feat, rows = features.shape
    sampled, edge_total = sample_row.shape[1], edge_src.shape[1]
    cap = 2 * sampled // groups
    low = min(512, rows, sampled)
    side = groups // HALVES
    width = weights.shape[2] // shares
    bf16, f32, i32 = jnp.bfloat16, jnp.float32, jnp.int32
    vmem = pl.BlockSpec(memory_space=pltpu.VMEM)
    any_space = pl.BlockSpec(memory_space=pl.ANY)
    dma = pltpu.SemaphoreType.DMA
    return pl.pallas_call(
        functools.partial(kernel, groups, shares),
        out_shape=jax.ShapeDtypeStruct((kinds, width, SEEDS), bf16),
        in_specs=[any_space] * 2 + [vmem] * 4 + [pl.BlockSpec(memory_space=pltpu.SMEM)],
        out_specs=vmem,
        scratch_shapes=[
            pltpu.VMEM(features.shape, bf16),
            pltpu.VMEM(weights.shape, bf16),
            dma((2,)),
            pltpu.VMEM((STEP, max(sampled, edge_total)), bf16),
            pltpu.VMEM((kinds, rows // low * feat, low), bf16),
            pltpu.VMEM((groups, kinds, cap), i32),
            pltpu.VMEM((groups, kinds, cap), i32),
            pltpu.VMEM((HALVES, kinds, sampled), i32),
            pltpu.VMEM((HALVES, RELS, edge_total), i32),
            pltpu.VMEM((kinds, side, HALVES, feat, cap), bf16),
            pltpu.VMEM((kinds, HALVES, side, feat, cap), bf16),
            pltpu.VMEM((HALVES, RELS, sampled, SEEDS), bf16),
            pltpu.VMEM((HALVES, RELS, 8, SEEDS), f32),
            pltpu.VMEM((MATS, feat, SEEDS), f32),
            pltpu.VMEM((HALVES, MATS, feat, SEEDS), bf16),
            pltpu.VMEM((HALVES, MATS, feat, SEEDS), bf16),
            pltpu.VMEM((shares, kinds, SEEDS, width), f32),
            pltpu.VMEM((shares, kinds, SEEDS, width), bf16),
            pltpu.VMEM((shares, kinds, SEEDS, width), bf16),
            dma((groups,)), dma((groups,)),
            dma((HALVES, 2)), dma((HALVES, 2)),
            dma((kinds, side, HALVES)), dma((kinds, side, HALVES)),
            dma((HALVES, kinds)), dma((HALVES, kinds)),
            dma((shares,)), dma((shares,)),
            dma((HALVES, RELS // CORES, 2)), dma((HALVES, RELS // CORES, 2)),
        ],
        compiler_params=pltpu.CompilerParams(
            collective_id=0, has_side_effects=True, vmem_limit_bytes=56 * 1024 * 1024),
    )(features, weights, sample_owner.transpose(0, 2, 1), sample_row, edge_src, edge_dst, edge_count.T)


def solution(mesh):
    return jax.shard_map(
        per_device,
        mesh=mesh,
        in_specs=(
            P(None, "mp", "dp"),
            P(None, "mp", None),
            P(None, "dp", None),
            P(None, "dp"),
            P(None, "dp"),
            P(None, "dp"),
            P(None, "dp"),
        ),
        out_specs=P(None, "mp", "dp"),
        check_vma=False,
    )
```
